32 devices in a mesh: ga: 2 (over core), band: 16 (over z, y, x).
Axes of the slice: x: 2, y: 2, z: 4, core: 2. Of those that a mesh axis runs over, the one named last changes fastest.
Arguments:
- orbitals: bfloat16 [1024, 2, 16384], P('band', None, 'ga'), may hold values from -6 to 6
- projectors: bfloat16 [864, 2, 16384], P(None, None, ('ga', 'band')), may hold values from -0.03125 to 0.03125
- coupling: float32 [4, 18, 18], replicated, may hold values from -6 to 6
- species: int32 [48], replicated, may hold values from 0 to 3
- offsets: int32 [48], replicated, may hold values from 0 to 846, as said below
Outputs:
- applied: bfloat16 [1024, 2, 16384], P('band', None, 'ga')
The draws below stay inside these ranges and needn't reach their ends.
Inputs may be any that keep to these rules, and one draw needn't show every extreme that they name: Each atom's 18 projectors are the 18 consecutive rows of projectors starting at its offset; offsets are multiples of 18, and the atoms' blocks are distinct and cover all 864 rows.
All inputs are finite; a program needn't handle non-finite values.
Results may differ from the reference program's by a relative error of at most 0.0049.
Values may be sent and summed in bfloat16 or wider, within the bound.
No kernel may reach another device: no remote copies, remote signals or barrier semaphores. Data moves between devices by JAX's collectives and lax.ppermute only.
A program may use at most 64 MiB of HBM per device.

```python
import jax
import jax.numpy as jnp
from jax import lax

NBANDS = 1024
PROJ = 18
NSP = 4
ATOMS = 48
NPW = 16384
NKB = 864


def draw_offsets(key, part):
    order = jax.random.permutation(key, ATOMS)
    return (order * PROJ).astype(jnp.int32)


def plant(drawn, stream_key, smallest, largest):
    extent = drawn.shape
    spot = [jax.random.randint(jax.random.fold_in(stream_key, axis), (), 0, extent[axis]) for axis in range(len(extent))]
    drawn = drawn.at[tuple(spot)].set(smallest)
    longest = extent.index(max(extent))
    spot[longest] = (spot[longest] + 1) % extent[longest]
    return drawn.at[tuple(spot)].set(largest)


def block_scale(key, dims, cuts, least, top_value):
    gain = 1.0
    for axis_at, blocks in cuts:
        heights = jax.random.uniform(jax.random.fold_in(jax.random.fold_in(key, 6), axis_at), (blocks,), jnp.float32, least / len(cuts), top_value / len(cuts))
        gain = gain * jnp.repeat(jnp.exp(heights), dims[axis_at] // blocks).reshape((-1,) + (1,) * (len(dims) - 1 - axis_at))
    return gain


def normal_values(stream_key, shape, spread, most, pieces=(), held_as=jnp.bfloat16):
    values = spread * jax.random.normal(stream_key, shape, jnp.float32)
    if pieces:
        values = values * block_scale(stream_key, shape, pieces, -0.22, 0.18)
    return jnp.clip(values, -most, most).astype(held_as)


def setup_inputs(seed: int = 0) -> dict:
    arg_keys = jax.random.split(jax.random.key(seed), 6)
    return {
        "orbitals": normal_values(arg_keys[0], (NBANDS, 2, NPW), 1.0, 6.0, ((0, 16), (2, 2))),
        "projectors": normal_values(arg_keys[1], (NKB, 2, NPW), (2 * NPW) ** -0.5, 0.03125, ((2, 32),)),
        "coupling": normal_values(arg_keys[2], (NSP, PROJ, PROJ), ((NPW / (18 * NKB)) ** 0.5), 6.0, (), jnp.float32),
        "species": plant(jax.random.randint(arg_keys[3], (ATOMS,), 0, NSP), jax.random.fold_in(arg_keys[3], 1), 0, NSP - 1).astype(jnp.int32),
        "offsets": draw_offsets(jax.random.fold_in(arg_keys[5], 71), 0),
    }


def reference(orbitals, projectors, coupling, species, offsets):
    total_proj = projectors.shape[0]
    total_bands = orbitals.shape[0]
    per_atom = coupling.shape[1]
    flat_proj = projectors.reshape(total_proj, -1)
    turned = jnp.concatenate([orbitals[:, 1, :], -orbitals[:, 0, :]], axis=1)
    stacked = jnp.concatenate([orbitals.reshape(total_bands, -1), turned], axis=0)
    becp = lax.dot_general(flat_proj, stacked, (((1,), (1,)), ((), ())), preferred_element_type=jnp.float32)
    becp = becp.reshape(ATOMS, per_atom, 2 * total_bands)
    blocks = (offsets // per_atom).astype(jnp.int32)
    atom_kind = jnp.zeros((ATOMS,), jnp.int32).at[blocks].set(species)
    matrices = coupling[atom_kind].astype(jnp.float32)
    dbecp = jnp.einsum("aij,ajc->aic", matrices, becp, precision=lax.Precision.HIGHEST)
    dbecp = dbecp.reshape(total_proj, 2 * total_bands).astype(jnp.bfloat16)
    real_part = lax.dot_general(dbecp, projectors[:, 0, :], (((0,), (0,)), ((), ())), preferred_element_type=jnp.float32)
    imag_part = lax.dot_general(dbecp, projectors[:, 1, :], (((0,), (0,)), ((), ())), preferred_element_type=jnp.float32)
    out_real = real_part[:total_bands] - imag_part[total_bands:]
    out_imag = imag_part[:total_bands] + real_part[total_bands:]
    return jnp.stack([out_real, out_imag], axis=1).astype(jnp.bfloat16)
```

```python
import jax
import jax.numpy as jnp
from jax import lax
from jax.sharding import PartitionSpec as P

SHARES = (24,)


def block_matrices(coupling, species, offsets):
    per_atom = coupling.shape[1]
    count = offsets.shape[0]
    blocks = jnp.arange(count, dtype=jnp.int32)
    matches = (offsets[None, :] == blocks[:, None] * per_atom).astype(jnp.int32)
    atom_kind = jnp.sum(matches * species[None, :], axis=1)
    onehot = (atom_kind[:, None] == jnp.arange(coupling.shape[0], dtype=jnp.int32)[None, :]).astype(
        jnp.float32
    )
    table = coupling.reshape(coupling.shape[0], per_atom * per_atom)
    picked = jnp.dot(
        onehot, table, precision=lax.Precision.HIGHEST, preferred_element_type=jnp.float32
    )
    return picked.reshape(count * per_atom, per_atom)


def block_diagonal(rows, per_atom):
    n = rows.shape[0]
    col = jnp.arange(n, dtype=jnp.int32)
    pick = (jnp.arange(per_atom, dtype=jnp.int32)[:, None] == (col % per_atom)[None, :]).astype(jnp.float32)
    wide = jnp.dot(rows, pick, precision=lax.Precision.HIGHEST, preferred_element_type=jnp.float32)
    return jnp.where((col // per_atom)[:, None] == (col // per_atom)[None, :], wide, 0.0)


def matmul(a, b, dims):
    return lax.dot_general(a, b, (dims, ((), ())), preferred_element_type=jnp.float32)


def build(n_ga, n_band):
    halves = 2 if n_band % 2 == 0 else 1
    group = n_band // halves
    groups = [list(range(h * group, (h + 1) * group)) for h in range(halves)]
    across = [(i, (i + group) % n_band) for i in range(n_band)]

    def ga_shift(x, k):
        return lax.ppermute(x, "ga", [(i, (i + k) % n_ga) for i in range(n_ga)])

    def exchange(x):
        return lax.all_to_all(x, "band", 0, 0, axis_index_groups=groups, tiled=True)

    def per_device(orbitals, projectors, coupling, species, offsets):
        bands, _, width = orbitals.shape
        total, _, piece = projectors.shape
        per_atom = coupling.shape[1]
        atoms = total // per_atom
        units = atoms // n_ga
        shares = SHARES if units == sum(SHARES) else (units,)
        starts = [n_ga * per_atom * sum(shares[:c]) for c in range(len(shares) + 1)]
        chunks = len(shares)
        lanes = 2 * bands
        ga = lax.axis_index("ga")
        side = lax.axis_index("band") // group

        own = [projectors[starts[c] : starts[c + 1]].reshape(-1, 2 * piece) for c in range(chunks)]
        held = [[f] for f in own]
        if halves == 2:
            for c in range(chunks):
                held[c].append(lax.ppermute(own[c], "band", across))

        orbitals, own = lax.optimization_barrier((orbitals, own))
        flat = orbitals.reshape(bands, 2, halves, group, piece)
        if halves == 2:
            flat = jnp.where(side == 0, flat, flat[:, :, ::-1])
        flat = flat.transpose(3, 0, 2, 1, 4).reshape(group, bands, halves * 2 * piece)
        spread = exchange(flat)
        stacked = []
        for h in range(halves):
            re = spread[:, :, 2 * h * piece : (2 * h + 1) * piece]
            im = spread[:, :, (2 * h + 1) * piece : (2 * h + 2) * piece]
            both = jnp.stack([jnp.concatenate([re, im], 2), jnp.concatenate([im, -re], 2)], axis=1)
            stacked.append(both.reshape(group * lanes, 2 * piece))

        kinds = block_matrices(coupling, species, offsets)
        real = [None] * halves
        imag = [None] * halves
        for c in range(chunks):
            part = shares[c] * per_atom
            value = matmul(held[c][0], stacked[0], ((1,), (1,)))
            for h in range(1, halves):
                value = value + matmul(held[c][h], stacked[h], ((1,), (1,)))
            value = value.reshape(n_ga, part, group * lanes)
            mine = lax.dynamic_index_in_dim(value, ga, 0, keepdims=False)
            for k in range(1, n_ga):
                other = lax.dynamic_index_in_dim(value, (ga + k) % n_ga, 0, keepdims=False)
                mine = mine + ga_shift(other, k)
            outgoing = mine.astype(jnp.bfloat16).reshape(part, group, lanes).transpose(1, 0, 2)
            becp = jnp.sum(exchange(outgoing).astype(jnp.float32), axis=0)
            rows_of = lax.dynamic_slice_in_dim(kinds, starts[c] + ga * part, part, 0)
            matrix = block_diagonal(rows_of, per_atom)
            dbecp = jnp.dot(
                matrix, becp, precision=lax.Precision.HIGHEST, preferred_element_type=jnp.float32
            ).astype(jnp.bfloat16)
            gathered = exchange(jnp.broadcast_to(dbecp[None], (group,) + dbecp.shape))
            gathered = gathered.transpose(1, 0, 2).reshape(part, group * lanes)
            pieces = [gathered] + [ga_shift(gathered, k) for k in range(1, n_ga)]
            columns = jnp.concatenate(pieces, axis=0)
            for h in range(halves):
                ranked = held[c][h].reshape(n_ga, part, 2 * piece)
                ranked = jnp.concatenate(
                    [lax.dynamic_index_in_dim(ranked, (ga - k) % n_ga, 0, keepdims=False) for k in range(n_ga)],
                    axis=0,
                )
                more_real = matmul(columns, ranked[:, :piece], ((0,), (0,)))
                more_imag = matmul(columns, ranked[:, piece:], ((0,), (0,)))
                real[h] = more_real if c == 0 else real[h] + more_real
                imag[h] = more_imag if c == 0 else imag[h] + more_imag

        sent = []
        for h in range(halves):
            r = real[h].reshape(group, 2, bands, piece)
            i = imag[h].reshape(group, 2, bands, piece)
            both = jnp.stack([r[:, 0] - i[:, 1], i[:, 0] + r[:, 1]], axis=1)
            sent.append(both.astype(jnp.bfloat16))
        got = exchange(jnp.stack(sent, axis=1))
        if halves == 2:
            got = jnp.where(side == 0, got, got[:, ::-1])
        return got.transpose(3, 2, 1, 0, 4).reshape(bands, 2, width)

    return per_device


def solution(mesh):
    placed = (P("band", None, "ga"), P(None, None, ("ga", "band")), P(), P(), P())
    return jax.shard_map(
        build(mesh.shape["ga"], mesh.shape["band"]),
        mesh=mesh,
        in_specs=placed,
        out_specs=P("band", None, "ga"),
        check_vma=False,
    )
```

```python
import jax
import jax.numpy as jnp
from jax import lax
from jax.sharding import PartitionSpec as P


SHARES = (24,)


def block_matrices(coupling, species, offsets):
    per_atom = coupling.shape[1]
    count = offsets.shape[0]
    blocks = jnp.arange(count, dtype=jnp.int32)
    matches = (offsets[None, :] == blocks[:, None] * per_atom).astype(jnp.int32)
    atom_kind = jnp.sum(matches * species[None, :], axis=1)
    onehot = (atom_kind[:, None] == jnp.arange(coupling.shape[0], dtype=jnp.int32)[None, :]).astype(
        jnp.float32
    )
    table = coupling.reshape(coupling.shape[0], per_atom * per_atom)
    picked = jnp.dot(
        onehot, table, precision=lax.Precision.HIGHEST, preferred_element_type=jnp.float32
    )
    return picked.reshape(count * per_atom, per_atom)


def block_diagonal(rows, per_atom):
    n = rows.shape[0]
    col = jnp.arange(n, dtype=jnp.int32)
    pick = (jnp.arange(per_atom, dtype=jnp.int32)[:, None] == (col % per_atom)[None, :]).astype(jnp.float32)
    wide = jnp.dot(rows, pick, precision=lax.Precision.HIGHEST, preferred_element_type=jnp.float32)
    return jnp.where((col // per_atom)[:, None] == (col // per_atom)[None, :], wide, 0.0)


def matmul(a, b, dims):
    return lax.dot_general(a, b, (dims, ((), ())), preferred_element_type=jnp.float32)


def build(n_ga, n_band):
    halves = 2 if n_band % 2 == 0 else 1
    group = n_band // halves
    groups = [list(range(h * group, (h + 1) * group)) for h in range(halves)]
    across = [(i, (i + group) % n_band) for i in range(n_band)]

    def ga_shift(x, k):
        return lax.ppermute(x, "ga", [(i, (i + k) % n_ga) for i in range(n_ga)])

    def exchange(x):
        return lax.all_to_all(x, "band", 0, 0, axis_index_groups=groups, tiled=True)

    def per_device(orbitals, projectors, coupling, species, offsets):
        bands, _, width = orbitals.shape
        total, _, piece = projectors.shape
        per_atom = coupling.shape[1]
        atoms = total // per_atom
        units = atoms // n_ga
        shares = SHARES if units == sum(SHARES) else (units,)
        starts = [n_ga * per_atom * sum(shares[:c]) for c in range(len(shares) + 1)]
        chunks = len(shares)
        lanes = 2 * bands
        ga = lax.axis_index("ga")
        side = lax.axis_index("band") // group

        own = [projectors[starts[c] : starts[c + 1]].reshape(-1, 2 * piece) for c in range(chunks)]
        held = [[f] for f in own]
        if halves == 2:
            for c in range(chunks):
                held[c].append(lax.ppermute(own[c], "band", across))

        orbitals, own = lax.optimization_barrier((orbitals, own))
        flat = orbitals.reshape(bands, 2, halves, group, piece)
        if halves == 2:
            flat = jnp.where(side == 0, flat, flat[:, :, ::-1])
        flat = flat.transpose(3, 0, 2, 1, 4).reshape(group, bands, halves * 2 * piece)
        spread = exchange(flat)
        stacked = []
        for h in range(halves):
            re = spread[:, :, 2 * h * piece : (2 * h + 1) * piece]
            im = spread[:, :, (2 * h + 1) * piece : (2 * h + 2) * piece]
            both = jnp.stack([jnp.concatenate([re, im], 2), jnp.concatenate([im, -re], 2)], axis=1)
            stacked.append(both.reshape(group * lanes, 2 * piece))

        kinds = block_matrices(coupling, species, offsets)
        real = [None] * halves
        imag = [None] * halves
        for c in range(chunks):
            part = shares[c] * per_atom
            value = matmul(held[c][0], stacked[0], ((1,), (1,)))
            for h in range(1, halves):
                value = value + matmul(held[c][h], stacked[h], ((1,), (1,)))
            value = value.reshape(n_ga, part, group * lanes)
            mine = lax.dynamic_index_in_dim(value, ga, 0, keepdims=False)
            for k in range(1, n_ga):
                other = lax.dynamic_index_in_dim(value, (ga + k) % n_ga, 0, keepdims=False)
                mine = mine + ga_shift(other, k)
            outgoing = mine.astype(jnp.bfloat16).reshape(part, group, lanes).transpose(1, 0, 2)
            arrived = exchange(outgoing)
            becp = jnp.sum(arrived.astype(jnp.float32), axis=0)
            rows_of = lax.dynamic_slice_in_dim(kinds, starts[c] + ga * part, part, 0)
            matrix = block_diagonal(rows_of, per_atom)
            dbecp = jnp.dot(
                matrix, becp, precision=lax.Precision.HIGHEST, preferred_element_type=jnp.float32
            ).astype(jnp.bfloat16)
            copies = jnp.broadcast_to(dbecp[None], (group,) + dbecp.shape)
            gathered = exchange(copies)
            gathered = gathered.transpose(1, 0, 2).reshape(part, group * lanes)
            pieces = [gathered] + [ga_shift(gathered, k) for k in range(1, n_ga)]
            columns = jnp.concatenate(pieces, axis=0)
            for h in range(halves):
                ranked = held[c][h].reshape(n_ga, part, 2 * piece)
                ranked = jnp.concatenate(
                    [lax.dynamic_index_in_dim(ranked, (ga - k) % n_ga, 0, keepdims=False) for k in range(n_ga)],
                    axis=0,
                )
                more_real = matmul(columns, ranked[:, :piece], ((0,), (0,)))
                more_imag = matmul(columns, ranked[:, piece:], ((0,), (0,)))
                real[h] = more_real if c == 0 else real[h] + more_real
                imag[h] = more_imag if c == 0 else imag[h] + more_imag

        sent = []
        for h in range(halves):
            r = real[h].reshape(group, 2, bands, piece)
            i = imag[h].reshape(group, 2, bands, piece)
            both = jnp.stack([r[:, 0] - i[:, 1], i[:, 0] + r[:, 1]], axis=1)
            sent.append(both.astype(jnp.bfloat16))
        got = exchange(jnp.stack(sent, axis=1))
        if halves == 2:
            got = jnp.where(side == 0, got, got[:, ::-1])
        return got.transpose(3, 2, 1, 0, 4).reshape(bands, 2, width)

    return per_device


def solution(mesh):
    placed = (P("band", None, "ga"), P(None, None, ("ga", "band")), P(), P(), P())
    inner = build(mesh.shape["ga"], mesh.shape["band"])

    return jax.shard_map(
        inner, mesh=mesh, in_specs=placed, out_specs=P("band", None, "ga"), check_vma=False
    )
```
